32 devices in a mesh: gx: 4 (over z), gy: 8 (over y, x, core).
Axes of the slice: x: 2, y: 2, z: 4, core: 2. Of those that a mesh axis runs over, the one named last changes fastest.
Arguments:
- node_coords: float32 [12288, 3, 128], P(('gx', 'gy')), may hold values from -6 to 6
- node_disp: float32 [12288, 3, 128], P(('gx', 'gy')), may hold values from -6 to 6
- qpoints: float32 [8192, 3, 256], P(('gx', 'gy')), may hold values from -6 to 6
- qweights: float32 [8192, 256], P(('gx', 'gy')), may hold values from 0.1 to 2
- qcount: int32 [8192], P(('gx', 'gy')), may hold values from 64 to 256
- sec_block: int32 [8192], P(('gx', 'gy')), may hold values from 0 to 12287, as said below
- pri_block: int32 [8192], P(('gx', 'gy')), may hold values from 0 to 12287, as said below
Outputs:
- gap: float32 [12288, 3, 128], P(('gx', 'gy'))
The draws below stay inside these ranges and needn't reach their ends.
Inputs may be any that keep to these rules, and one draw needn't show every extreme that they name: `sec_block`: patch b is owned by device b // 384. Among the segments of one device, at most 16 have their secondary patch owned by any one device; in every draw some device owns the secondary patches of exactly 16 segments of every device. `pri_block`: as for sec_block, with primary patches: at most 16 segments of one device name patches of any one owner, and some owner gets exactly 16 from every device.
All inputs are finite; a program needn't handle non-finite values.
Results may differ from the reference program's by a relative error of at most 0.000098.
Values sent between devices are 32-bit elements; how exact they have to be, the bound alone decides.
A program may use at most 64 MiB of HBM per device.

```python
import math
import jax
import jax.numpy as jnp
from jax import lax

NPB = 128
Q = 256
SEG_DEV = 256
NB_DEV = 384
NDEV = 32
CAP = 16
SEGMENTS = 8192
NB = 12288


def owner_routes(key):
    slot_count = NDEV * CAP
    hot_owner = jax.random.randint(jax.random.fold_in(key, 5), (), 0, NDEV)
    device_keys = jax.random.split(jax.random.fold_in(key, 7), NDEV)

    def one_device(dev_key):
        first, second, third = jax.random.split(dev_key, 3)
        positions = jnp.arange(slot_count, dtype=jnp.int32)
        scores = jax.random.randint(first, (slot_count,), 0, 65536) * slot_count + positions
        scores = jnp.where(positions // CAP == hot_owner, scores + 2 ** 30, scores)
        chosen = jax.lax.top_k(scores, SEG_DEV)[1]
        owners = (chosen // CAP).astype(jnp.int32)
        owners = jax.random.permutation(second, owners)
        local_ids = jax.random.randint(third, (SEG_DEV,), 0, NB_DEV)
        return owners * NB_DEV + local_ids
    return jax.vmap(one_device)(device_keys).reshape(-1).astype(jnp.int32)


def draw_sec_block(key, part):
    return owner_routes(jax.random.fold_in(key, 11))


def draw_pri_block(key, part):
    return owner_routes(jax.random.fold_in(key, 23))


def set_ends(array, key, least, high):
    longest = array.shape.index(max(array.shape))
    spots = []
    for shift in (0, 1):
        where = [jax.random.randint(jax.random.fold_in(key, axis), (), 0, length) for axis, length in enumerate(array.shape)]
        where[longest] = (where[longest] + shift) % array.shape[longest]
        spots.append(tuple(where))
    return array.at[spots[0]].set(least).at[spots[1]].set(high)


def levels(stream_key, dims, cuts, smallest, largest):
    gain = 1.0
    for dim, blocks in cuts:
        steps = jax.random.uniform(jax.random.fold_in(jax.random.fold_in(stream_key, 6), dim), (blocks,), jnp.float32, smallest / len(cuts), largest / len(cuts))
        gain = gain * jnp.repeat(jnp.exp(steps), dims[dim] // blocks).reshape((-1,) + (1,) * (len(dims) - 1 - dim))
    return gain


def normal_values(key, shape, width, limit, pieces=(), kind=jnp.bfloat16):
    values = jax.random.normal(key, shape, jnp.float32) * width
    if len(pieces) > 0:
        values = levels(key, shape, pieces, -0.22, 0.18) * values
    return jnp.clip(values, min=-limit, max=limit).astype(kind)


def setup_inputs(seed: int = 0) -> dict:
    keys = jax.random.split(jax.random.key(seed), 8)
    node_coords = normal_values(keys[0], (NB, 3, NPB), 1.0, 6.0, ((0, 32),), jnp.float32)
    node_disp = normal_values(keys[1], (NB, 3, NPB), 1.0, 6.0, ((0, 32),), jnp.float32)
    qpoints = normal_values(keys[2], (SEGMENTS, 3, Q), 1.0, 6.0, ((0, 32),), jnp.float32)
    qweights = jnp.clip(jnp.exp(math.log(2.0) - 2.9957323 * jax.random.uniform(keys[3], (SEGMENTS, Q), jnp.float32) ** levels(keys[3], (SEGMENTS, Q), ((0, 32),), -0.2, 0.2)), 0.1, 2.0)
    qcount = set_ends(jax.random.randint(keys[4], (SEGMENTS,), Q // 4, Q + 1), jax.random.fold_in(keys[4], 1), Q // 4, Q).astype(jnp.int32)
    sec_block = draw_sec_block(jax.random.fold_in(keys[7], 71), 0)
    pri_block = draw_pri_block(jax.random.fold_in(keys[7], 71), 0)
    return {"node_coords": node_coords, "node_disp": node_disp, "qpoints": qpoints, "qweights": qweights, "qcount": qcount, "sec_block": sec_block, "pri_block": pri_block}


def shape_values(points, coords):
    diff0 = points[:, 0, :, None] - coords[:, 0, None, :]
    diff1 = points[:, 1, :, None] - coords[:, 1, None, :]
    diff2 = points[:, 2, :, None] - coords[:, 2, None, :]
    radius = diff0 * diff0 + diff1 * diff1 + diff2 * diff2
    kernel = 1.0 / (1.0 + 2.0 * radius)
    return kernel / jnp.sum(kernel, axis=-1, keepdims=True)


def reference(node_coords, node_disp, qpoints, qweights, qcount, sec_block, pri_block):
    node_data = jnp.concatenate([node_coords, node_disp], axis=1)
    live = jnp.arange(Q, dtype=jnp.int32)[None, :] < qcount[:, None]
    weights = jnp.where(live, qweights, jnp.zeros_like(qweights))
    seg_group = 64
    groups = SEGMENTS // seg_group
    hp = lax.Precision.HIGHEST

    def one_group(inputs):
        points, quad_weights, sec_ids, pri_ids = inputs
        sec_nodes = jnp.take(node_data, sec_ids, axis=0)
        pri_nodes = jnp.take(node_data, pri_ids, axis=0)
        sec_shape = shape_values(points, sec_nodes[:, :3])
        pri_shape = shape_values(points, pri_nodes[:, :3])
        weighted = quad_weights[:, :, None] * sec_shape
        mismatch = jnp.einsum("gqj,gcj->gcq", sec_shape, sec_nodes[:, 3:], precision=hp) - jnp.einsum("gqj,gcj->gcq", pri_shape, pri_nodes[:, 3:], precision=hp)
        return jnp.einsum("gqk,gcq->gck", weighted, mismatch, precision=hp)

    contrib = lax.map(one_group, (qpoints.reshape(groups, seg_group, 3, Q), weights.reshape(groups, seg_group, Q), sec_block.reshape(groups, seg_group), pri_block.reshape(groups, seg_group)))
    contrib = contrib.reshape(SEGMENTS, 3, NPB)
    return jax.ops.segment_sum(contrib, sec_block, num_segments=NB)
```

```python
import functools
import jax
import jax.numpy as jnp
from jax import lax
from jax.experimental import pallas as pl
from jax.experimental.pallas import tpu as pltpu
from jax.sharding import PartitionSpec as P

GROUP = 16
CHUNKS = 2
F32, BF16 = jnp.float32, jnp.bfloat16
MESH = pl.DeviceIdType.MESH


def ranks_of(owners):
    positions = jnp.arange(owners.shape[0], dtype=jnp.int32)
    same = (owners[:, None] == owners[None, :]) & (positions[:, None] > positions[None, :])
    return jnp.sum(same.astype(jnp.int32), axis=1)


def pick(values, where, size, empty):
    match = where[:, None] == jnp.arange(size, dtype=jnp.int32)[None, :]
    return jnp.sum(jnp.where(match, (values - empty)[:, None], 0), axis=0) + empty


def exchange(x):
    return lax.all_to_all(x, ("gx", "gy"), split_axis=0, concat_axis=0, tiled=True)


def rounded(x):
    return x.astype(BF16).astype(F32)


def stack_rows(rows, iota):
    out = jnp.zeros(iota.shape, F32)
    for i, row in rows:
        out = jnp.where(iota == i, row, out)
    return out


def disp_rows(row, n):
    iota = lax.broadcasted_iota(jnp.int32, (8, n), 0)
    u = [row[:, (3 + c) * n : (4 + c) * n] for c in range(3)]
    full = stack_rows([(i + 4 * h, u[i]) for h in range(2) for i in range(3)], iota)
    full = jnp.where((iota == 3) | (iota == 7), 1.0, full)
    both = jnp.where(iota < 4, rounded(full), full - rounded(full)).astype(BF16)
    return jnp.concatenate([both, both], axis=1)


def split_three(full):
    high = rounded(full)
    rest = full - high
    mid = rounded(rest)
    return high, mid, rest - mid


def point_features(qp, s):
    iota = lax.broadcasted_iota(jnp.int32, (8, qp.shape[2]), 0)
    x = [qp[c, pl.ds(s, 1), :] for c in range(3)]
    square = 1.0 + 2.0 * (x[0] * x[0] + x[1] * x[1] + x[2] * x[2])
    full = stack_rows([(0, x[0]), (1, x[1]), (2, x[2]), (3, 1.0), (4, square)], iota)
    high, mid, low = split_three(full)
    return jnp.concatenate([high, mid, high, low, high, mid], axis=0).astype(BF16)


def kernel_values(row, feat, n):
    iota = lax.broadcasted_iota(jnp.int32, (8, n), 0)
    x = [row[:, c * n : (c + 1) * n] for c in range(3)]
    square = 2.0 * (x[0] * x[0] + x[1] * x[1] + x[2] * x[2])
    full = stack_rows(
        [(0, -4.0 * x[0]), (1, -4.0 * x[1]), (2, -4.0 * x[2]), (3, square), (4, 1.0)], iota
    )
    high, mid, low = split_three(full)
    left = jnp.concatenate([high, high, mid, high, low, mid], axis=0)
    kern = 1.0 / jnp.dot(left.T.astype(BF16), feat, preferred_element_type=F32)
    kh = kern.astype(BF16)
    return kh, (kern - kh.astype(F32)).astype(BF16)


def fused_kernel(
    pri_ids, sec_ids, pri_slots, sec_slots, order, inverse, counts,
    hot_ids, coords, disp, qp, weights, gap,
    pri_send, pri_recv, sec_send, means, parcels, both_s, gap_s, *rest,
):
    chunks = sec_send.shape[0]
    sec_recv, rest = rest[:chunks], rest[chunks:]
    par_send, rest = rest[:chunks], rest[chunks:]
    par_recv, rest = rest[:chunks], rest[chunks:]
    send_sem, recv_sem = rest
    ny = lax.axis_size("gy")
    devices, cap, width = pri_send.shape
    cap_c = sec_send.shape[2]
    n = width // 6
    segs = means.shape[0]
    points = qp.shape[2]
    me = lax.axis_index("gx") * ny + lax.axis_index("gy")

    def partner(t):
        return lax.rem(me + t, devices)

    def place(p):
        return (p // ny, lax.rem(p, ny))

    def copy(src, dst, k, t):
        p = partner(t)
        return pltpu.make_async_remote_copy(
            src_ref=src.at[p],
            dst_ref=dst.at[me],
            send_sem=send_sem.at[k, t],
            recv_sem=recv_sem.at[k, t],
            device_id=place(p),
            device_id_type=MESH,
        )

    half = devices // 2

    def far_first(i):
        t = i + half
        return jnp.where(t >= devices, t - devices + 1, t)

    def start_all(src, dst, k):
        @pl.loop(0, devices - 1)
        def _(i):
            copy(src, dst, k, far_first(i)).start()

    def wait_recv(src, dst, k):
        @pl.loop(1, devices)
        def _(t):
            copy(src, dst, k, t).wait_recv()

    def wait_send(src, dst, k):
        @pl.loop(1, devices)
        def _(t):
            copy(src, dst, k, t).wait_send()

    def gather(ids, base, dst, p, rows):
        for j in range(rows):
            b = ids[base + j]
            for c in range(3):
                dst[p, j : j + 1, c * n : (c + 1) * n] = coords[c, pl.ds(b, 1), :]
                k = 3 + c
                dst[p, j : j + 1, k * n : (k + 1) * n] = disp[c, pl.ds(b, 1), :]

    def lift(i, c, dst, p):
        base = (c * devices + p) * cap_c
        for j in range(cap_c):
            k = inverse[base + j]
            for d in range(3):
                dst[p, j : j + 1, d * n : (d + 1) * n] = parcels[k, d : d + 1, :]

    barrier = pltpu.get_barrier_semaphore()

    @pl.loop(1, devices)
    def _(t):
        pl.semaphore_signal(barrier, inc=1, device_id=place(partner(t)), device_id_type=MESH)

    @pl.loop(0, devices - 1)
    def _(i):
        p = partner(far_first(i))
        gather(pri_ids, p * cap, pri_send, p, cap)

    gather(pri_ids, me * cap, pri_recv, me, cap)
    pl.semaphore_wait(barrier, devices - 1)
    start_all(pri_send, pri_recv, 0)
    for c in range(chunks):

        @pl.loop(0, devices - 1)
        def _(i):
            p = partner(far_first(i))
            gather(sec_ids, (c * devices + p) * cap_c, sec_send.at[c], p, cap_c)

        gather(sec_ids, (c * devices + me) * cap_c, sec_recv[c], me, cap_c)
        start_all(sec_send.at[c], sec_recv[c], 1 + c)

    def group_values(nodes, slot_of, seg_of):
        for g in range(GROUP):
            slot = slot_of(g)
            row = nodes[slot // nodes.shape[1], pl.ds(lax.rem(slot, nodes.shape[1]), 1), :]
            kh, kl = kernel_values(row, point_features(qp, seg_of(g)), n)
            both_s[g, :n] = kh
            both_s[g, n:] = kl

    def group_mean(nodes, slot):
        row = nodes[slot // nodes.shape[1], pl.ds(lax.rem(slot, nodes.shape[1]), 1), :]
        return disp_rows(row, n)

    def mean_of(lhs, g):
        a = jnp.dot(lhs, both_s[g], preferred_element_type=F32)
        total = a + pltpu.roll(a, 4, 0)
        inv = 1.0 / total[3:4]
        return total * inv, inv

    wait_recv(pri_send, pri_recv, 0)

    @pl.loop(0, segs // GROUP)
    def _(i):
        group_values(pri_recv, lambda g: pri_slots[i * GROUP + g], lambda g: i * GROUP + g)
        for g in range(GROUP):
            s = i * GROUP + g
            means[s] = mean_of(group_mean(pri_recv, pri_slots[s]), g)[0]

    parcels[segs] = jnp.zeros(parcels.shape[1:], F32)
    iota = lax.broadcasted_iota(jnp.int32, (8, points), 0)
    lane = lax.broadcasted_iota(jnp.int32, (1, points), 1)
    steps = segs // chunks // GROUP
    for c in range(chunks):
        nodes = sec_recv[c]
        wait_recv(sec_send.at[c], nodes, 1 + c)

        @pl.loop(c * steps, (c + 1) * steps)
        def _(i):
            group_values(nodes, lambda g: sec_slots[i * GROUP + g], lambda g: order[i * GROUP + g])
            for g in range(GROUP):
                s = order[i * GROUP + g]
                mean, inv = mean_of(group_mean(nodes, sec_slots[i * GROUP + g]), g)
                w = jnp.where(lane < counts[s], weights[pl.ds(s, 1), :], 0.0)
                diff = (mean - means[s]) * (w * inv)
                high = rounded(diff)
                gap_s[g] = jnp.where(iota < 4, high, diff - high)
            for g in range(GROUP):
                y = lax.dot_general(
                    gap_s[g].astype(BF16), both_s[g], (((1,), (1,)), ((), ())),
                    preferred_element_type=F32,
                )
                y = y[:, :n] + y[:, n:]
                parcels[i * GROUP + g] = y + pltpu.roll(y, 4, 0)

        @pl.loop(0, devices - 1)
        def _(i):
            lift(i, c, par_send[c], partner(far_first(i)))

        lift(0, c, par_recv[c], me)
        start_all(par_send[c], par_recv[c], 1 + chunks + c)

    wait_send(pri_send, pri_recv, 0)
    for c in range(chunks):
        wait_send(sec_send.at[c], sec_recv[c], 1 + c)
    blocks = gap.shape[1]
    slots_c = devices * cap_c
    for c in range(chunks):
        wait_recv(par_send[c], par_recv[c], 1 + chunks + c)
        match = lax.broadcasted_iota(jnp.int32, (blocks, slots_c), 0) == hot_ids[c : c + 1]
        select = jnp.where(match, 1.0, 0.0).astype(BF16)
        for d in range(3):
            x = par_recv[c][:, :, d * n : (d + 1) * n].reshape(slots_c, n)
            high, mid, low = split_three(x)
            pieces = jnp.concatenate([high, mid, low], axis=1).astype(BF16)
            y = jnp.dot(select, pieces, preferred_element_type=F32)
            y = y[:, :n] + (y[:, n : 2 * n] + y[:, 2 * n :])
            gap[d] = y if c == 0 else gap[d] + y
    for c in range(chunks):
        wait_send(par_send[c], par_recv[c], 1 + chunks + c)


def fused(tables, hot_ids, coords, disp, qp, weights, devices, cap, chunks):
    comps, blocks, n = coords.shape
    _, segs, points = qp.shape
    cap_c = cap // chunks
    width = 2 * comps * n
    vmem, smem = pl.BlockSpec(memory_space=pltpu.VMEM), pl.BlockSpec(memory_space=pltpu.SMEM)
    nodes_c = [pltpu.VMEM((devices, cap_c, width), F32) for _ in range(chunks)]
    parts_c = [pltpu.VMEM((devices, cap_c, comps * n), F32) for _ in range(2 * chunks)]
    kinds = 1 + 2 * chunks
    return pl.pallas_call(
        fused_kernel,
        out_shape=jax.ShapeDtypeStruct((comps, blocks, n), F32),
        in_specs=[smem] * len(tables) + [vmem] * 5,
        out_specs=vmem,
        scratch_shapes=[
            pltpu.VMEM((devices, cap, width), F32),
            pltpu.VMEM((devices, cap, width), F32),
            pltpu.VMEM((chunks, devices, cap_c, width), F32),
            pltpu.VMEM((segs, 8, points), F32),
            pltpu.VMEM((segs + 1, 8, n), F32),
            pltpu.VMEM((GROUP, 2 * n, points), BF16),
            pltpu.VMEM((GROUP, 8, points), F32),
            *nodes_c,
            *parts_c,
            pltpu.SemaphoreType.DMA((kinds, devices)),
            pltpu.SemaphoreType.DMA((kinds, devices)),
        ],
        compiler_params=pltpu.CompilerParams(collective_id=0, has_side_effects=True),
        name="fused",
    )(*tables, hot_ids, coords, disp, qp, weights)


def body(node_coords, node_disp, qpoints, qweights, qcount, sec_block, pri_block):
    devices = lax.axis_size("gx") * lax.axis_size("gy")
    blocks = node_coords.shape[0]
    segs = qpoints.shape[0]
    cap = 2 * segs // devices
    chunks = CHUNKS
    cap_c = cap // chunks
    slots, slots_c = devices * cap, devices * cap_c
    pri_owner, sec_owner = pri_block // blocks, sec_block // blocks
    pri_slot = pri_owner * cap + ranks_of(pri_owner)
    pri_request = pick(pri_block % blocks, pri_slot, slots, 0)
    rank = ranks_of(sec_owner)
    start = jnp.sum((sec_owner[:, None] > sec_owner[None, :]).astype(jnp.int32), axis=1)
    position = start + rank
    chunk = position % chunks
    turn = chunk * (segs // chunks) + position // chunks
    slot_c = sec_owner * cap_c + rank // chunks
    place = chunk * slots_c + slot_c
    sec_request = pick(sec_block % blocks, place, slots, 0)
    inverse = pick(turn, place, slots, segs)
    order = pick(jnp.arange(segs, dtype=jnp.int32), turn, segs, 0)
    sec_slot = pick(slot_c, turn, segs, 0)
    sec_rows = sec_request.reshape(chunks, devices, cap_c).transpose(1, 0, 2)
    requests = jnp.stack([pri_request.reshape(devices, cap), sec_rows.reshape(devices, cap)], axis=1)
    received = exchange(requests)
    pri_ids = received[:, 0].reshape(slots)
    sec_ids = received[:, 1].reshape(devices, chunks, cap_c).transpose(1, 0, 2).reshape(slots)
    tables = (pri_ids, sec_ids, pri_slot, sec_slot, order, inverse, qcount)
    gap = fused(
        tables,
        sec_ids.reshape(chunks, slots_c),
        node_coords.transpose(1, 0, 2),
        node_disp.transpose(1, 0, 2),
        qpoints.transpose(1, 0, 2),
        qweights,
        devices,
        cap,
        chunks,
    )
    return gap.transpose(1, 0, 2)


def solution(mesh):
    placed = (
        P(("gx", "gy"), None, None),
        P(("gx", "gy"), None, None),
        P(("gx", "gy"), None, None),
        P(("gx", "gy"), None),
        P(("gx", "gy")),
        P(("gx", "gy")),
        P(("gx", "gy")),
    )
    return jax.shard_map(
        body, mesh=mesh, in_specs=placed, out_specs=P(("gx", "gy"), None, None), check_vma=False
    )
```

```python
import functools
import jax
import jax.numpy as jnp
from jax import lax
from jax.experimental import pallas as pl
from jax.experimental.pallas import tpu as pltpu
from jax.sharding import PartitionSpec as P

GROUP = 16
PHASES = (2, 1, 1)
F32, BF16 = jnp.float32, jnp.bfloat16
MESH = pl.DeviceIdType.MESH


def rounded(x):
    return x.astype(BF16).astype(F32)


def stack_rows(rows, iota):
    out = jnp.zeros(iota.shape, F32)
    for i, row in rows:
        out = jnp.where(iota == i, row, out)
    return out


def disp_rows(row, n):
    iota = lax.broadcasted_iota(jnp.int32, (8, n), 0)
    u = [row[:, (3 + c) * n : (4 + c) * n] for c in range(3)]
    full = stack_rows([(i + 4 * h, u[i]) for h in range(2) for i in range(3)], iota)
    full = jnp.where((iota == 3) | (iota == 7), 1.0, full)
    both = jnp.where(iota < 4, rounded(full), full - rounded(full)).astype(BF16)
    return jnp.concatenate([both, both], axis=1)


def split_three(full):
    high = rounded(full)
    rest = full - high
    mid = rounded(rest)
    return high, mid, rest - mid


def point_features(qp, s):
    iota = lax.broadcasted_iota(jnp.int32, (8, qp.shape[2]), 0)
    x = [qp[c, pl.ds(s, 1), :] for c in range(3)]
    square = 1.0 + 2.0 * (x[0] * x[0] + x[1] * x[1] + x[2] * x[2])
    full = stack_rows([(0, x[0]), (1, x[1]), (2, x[2]), (3, 1.0), (4, square)], iota)
    high, mid, low = split_three(full)
    return jnp.concatenate([high, mid, high, low, high, mid], axis=0).astype(BF16)


def kernel_values(row, feat, n):
    iota = lax.broadcasted_iota(jnp.int32, (8, n), 0)
    x = [row[:, c * n : (c + 1) * n] for c in range(3)]
    square = 2.0 * (x[0] * x[0] + x[1] * x[1] + x[2] * x[2])
    full = stack_rows(
        [(0, -4.0 * x[0]), (1, -4.0 * x[1]), (2, -4.0 * x[2]), (3, square), (4, 1.0)], iota
    )
    high, mid, low = split_three(full)
    left = jnp.concatenate([high, high, mid, high, low, mid], axis=0)
    kern = 1.0 / jnp.dot(left.T.astype(BF16), feat, preferred_element_type=F32)
    kh = kern.astype(BF16)
    return kh, (kern - kh.astype(F32)).astype(BF16)


def floor_div(x, m):
    return jnp.floor((x + 0.5) * (1.0 / m))


def whole(x, size):
    return jnp.clip(x.astype(jnp.int32), 0, size - 1)


def one_hot_sum(lhs, match):
    return lax.dot_general(
        lhs.astype(BF16), jnp.where(match, 1.0, 0.0).astype(BF16), (((1,), (1,)), ((), ())),
        preferred_element_type=F32,
    )


def sixteens(x):
    high = jnp.floor(x * 0.0625)
    return high, x - 16.0 * high


def owners_of(block, blocks, cap):
    segs = block.shape[1]
    owner = floor_div(block, blocks)
    across = jnp.broadcast_to(owner, (segs, segs))
    down = across.T
    before = lax.broadcasted_iota(jnp.int32, (segs, segs), 0) < lax.broadcasted_iota(
        jnp.int32, (segs, segs), 1
    )
    same = jnp.where((down == across) & before, 1.0, 0.0)
    rank = jnp.sum(same, axis=0, keepdims=True)
    start = jnp.sum(jnp.where(down < across, 1.0, 0.0), axis=0, keepdims=True)
    return owner, block - owner * blocks, rank, start


def deal(owner, rank, start, segs, devices, cap):
    total = sum(PHASES)
    quarter = cap // total
    position = start + rank
    phase = position - total * floor_div(position, total)
    turn = place = slot = lane = jnp.zeros_like(owner)
    first = 0
    for count in PHASES:

        def before(x):
            turns = floor_div(x, total)
            return turns * count + jnp.clip(x - total * turns - first, 0.0, count)

        inside = (phase >= first) & (phase < first + count)
        spot = before(position)
        nth = spot - before(start)
        here = owner * (count * quarter) + nth
        turn = jnp.where(inside, spot + first * (segs // total), turn)
        slot = jnp.where(inside, here, slot)
        place = jnp.where(inside, here + first * quarter * devices, place)
        lane = jnp.where(inside, nth + (cap + first * quarter), lane)
        first += count
    return turn, slot, place, lane


def fused_kernel(
    pri_block, sec_block, counts, coords, disp, qp, weights, gap,
    req_send, req_recv, req_rows, ids, table_v, table, hot,
    pri_send, pri_recv, means, parcels, both_s, gap_s, *rest,
):
    chunks = len(PHASES)
    sec_send, rest = rest[:chunks], rest[chunks:]
    sec_recv, rest = rest[:chunks], rest[chunks:]
    par_send, rest = rest[:chunks], rest[chunks:]
    par_recv, rest = rest[:chunks], rest[chunks:]
    send_sem, recv_sem, local_sem = rest
    ny = lax.axis_size("gy")
    devices, cap, width = pri_send.shape
    n = width // 6
    segs, points = weights.shape
    blocks = coords.shape[1]
    slots = devices * cap
    total = sum(PHASES)
    quarter = cap // total
    firsts = [sum(PHASES[:c]) for c in range(chunks)]
    caps = [m * quarter for m in PHASES]
    me = lax.axis_index("gx") * ny + lax.axis_index("gy")

    def partner(t):
        return lax.rem(me + t, devices)

    def device(p):
        return (p // ny, lax.rem(p, ny))

    def copy(src, dst, k, t):
        p = partner(t)
        return pltpu.make_async_remote_copy(
            src_ref=src.at[p],
            dst_ref=dst.at[me],
            send_sem=send_sem.at[k, t],
            recv_sem=recv_sem.at[k, t],
            device_id=device(p),
            device_id_type=MESH,
        )

    half = devices // 2

    def far_first(i):
        t = i + half
        return jnp.where(t >= devices, t - devices + 1, t)

    def fill_and_start(fill, src, dst, k):
        fill(partner(far_first(0)), src)

        @pl.loop(1, devices - 1)
        def _(i):
            fill(partner(far_first(i)), src)
            copy(src, dst, k, far_first(i - 1)).start()

        fill(me, dst)
        copy(src, dst, k, far_first(devices - 2)).start()

    def wait_recv(src, dst, k):
        @pl.loop(1, devices)
        def _(t):
            copy(src, dst, k, t).wait_recv()

    def wait_send(src, dst, k):
        @pl.loop(1, devices)
        def _(t):
            copy(src, dst, k, t).wait_send()

    barrier = pltpu.get_barrier_semaphore()

    @pl.loop(1, devices)
    def _(t):
        pl.semaphore_signal(barrier, inc=1, device_id=device(partner(t)), device_id_type=MESH)

    pri = pri_block[...].reshape(1, segs).astype(F32)
    sec = sec_block[...].reshape(1, segs).astype(F32)
    pri_owner, pri_local, pri_rank, _ = owners_of(pri, blocks, cap)
    sec_owner, sec_local, sec_rank, sec_start = owners_of(sec, blocks, cap)
    turn, slot, place, lane = deal(sec_owner, sec_rank, sec_start, segs, devices, cap)
    owner = jnp.concatenate([pri_owner, sec_owner], axis=1)
    column = jnp.concatenate([pri_rank, lane], axis=1)
    local = jnp.concatenate([pri_local, sec_local], axis=1)
    to_owner = lax.broadcasted_iota(jnp.int32, (devices, 2 * segs), 0).astype(F32) == owner
    to_owner = jnp.where(to_owner, 1.0, 0.0)
    at_lane = lax.broadcasted_iota(jnp.int32, (128, 2 * segs), 0).astype(F32) == column
    pieces = [
        lax.dot_general(
            to_owner.astype(BF16), jnp.where(at_lane, part, 0.0).astype(BF16),
            (((1,), (1,)), ((), ())), preferred_element_type=F32,
        )
        for part in sixteens(local)
    ]
    req_rows[...] = 16.0 * pieces[0] + pieces[1]

    @pl.loop(0, devices)
    def _(p):
        req_send[p] = whole(req_rows[pl.ds(p, 1), :], blocks)

    req_recv[me] = whole(req_rows[pl.ds(me, 1), :], blocks)
    pl.semaphore_wait(barrier, devices - 1)

    @pl.loop(0, devices - 1)
    def _(i):
        copy(req_send, req_recv, 0, far_first(i)).start()

    number = lax.broadcasted_iota(jnp.int32, (1, segs), 1).astype(F32)
    zero = jnp.zeros((4, segs), F32)
    rows = jnp.concatenate([*sixteens(number), *sixteens(slot), zero], axis=0)
    match = lax.broadcasted_iota(jnp.int32, (segs, segs), 0).astype(F32) == turn
    found = one_hot_sum(rows, match)
    rows = jnp.concatenate([*sixteens(turn + 1.0), zero, zero[:2]], axis=0)
    match = lax.broadcasted_iota(jnp.int32, (slots, segs), 0).astype(F32) == place
    inverse = one_hot_sum(rows, match)
    inverse = 16.0 * inverse[0:1] + inverse[1:2] - 1.0
    inverse = jnp.where(inverse < 0.0, float(segs), inverse)
    turns = lax.broadcasted_iota(jnp.int32, (1, segs), 1)
    sizes = jnp.zeros_like(turns)
    for c in range(chunks):
        sizes = jnp.where(turns >= firsts[c] * (segs // total), devices * caps[c], sizes)
    table_v[0:1, :segs] = whole(pri_owner * cap + pri_rank, slots)
    table_v[1:2, :segs] = whole(16.0 * found[0:1] + found[1:2], segs)
    table_v[2:3, :segs] = whole(16.0 * found[2:3] + found[3:4], sizes)
    table_v[3:4, :] = whole(inverse, segs + 1)
    load_table = pltpu.make_async_copy(table_v, table, local_sem.at[0])
    load_table.start()

    wait_recv(req_send, req_recv, 0)
    load_ids = pltpu.make_async_copy(req_recv, ids, local_sem.at[1])
    load_ids.start()
    load_table.wait()
    load_ids.wait()

    def gather(base, count, p, dst):
        for j in range(count):
            b = ids[p, 0, base + j]
            for c in range(3):
                dst[p, j : j + 1, c * n : (c + 1) * n] = coords[c, pl.ds(b, 1), :]
                k = 3 + c
                dst[p, j : j + 1, k * n : (k + 1) * n] = disp[c, pl.ds(b, 1), :]

    fill_and_start(functools.partial(gather, 0, cap), pri_send, pri_recv, 1)
    for c in range(chunks):
        fill = functools.partial(gather, cap + firsts[c] * quarter, caps[c])
        fill_and_start(fill, sec_send[c], sec_recv[c], 2 + c)

    @pl.loop(0, devices)
    def _(p):
        req_rows[pl.ds(p, 1), :] = req_recv[p].astype(F32)

    high, low = sixteens(req_rows[...])
    for c in range(chunks):
        size = devices * caps[c]
        k = lax.broadcasted_iota(jnp.int32, (1, size), 1).astype(F32)
        from_row = floor_div(k, caps[c])
        from_lane = k - from_row * caps[c] + float(cap + firsts[c] * quarter)
        spread = lax.broadcasted_iota(jnp.int32, (128, size), 0).astype(F32) == from_lane
        spread = jnp.where(spread, 1.0, 0.0).astype(BF16)
        y = 16.0 * jnp.dot(high.astype(BF16), spread, preferred_element_type=F32)
        y = y + jnp.dot(low.astype(BF16), spread, preferred_element_type=F32)
        mine = lax.broadcasted_iota(jnp.int32, (devices, size), 0).astype(F32) == from_row
        hot[c : c + 1, :size] = jnp.sum(jnp.where(mine, y, 0.0), axis=0, keepdims=True)

    def row_of(nodes, spot):
        return nodes[spot // nodes.shape[1], pl.ds(lax.rem(spot, nodes.shape[1]), 1), :]

    def group_values(nodes, slot_of, seg_of):
        for g in range(GROUP):
            kh, kl = kernel_values(row_of(nodes, slot_of(g)), point_features(qp, seg_of(g)), n)
            both_s[g, :n] = kh
            both_s[g, n:] = kl

    def mean_of(row, g):
        a = jnp.dot(disp_rows(row, n), both_s[g], preferred_element_type=F32)
        sums = a + pltpu.roll(a, 4, 0)
        inv = 1.0 / sums[3:4]
        return sums * inv, inv

    wait_recv(pri_send, pri_recv, 1)

    @pl.loop(0, segs // GROUP)
    def _(i):
        group_values(pri_recv, lambda g: table[0, i * GROUP + g], lambda g: i * GROUP + g)
        for g in range(GROUP):
            s = i * GROUP + g
            means[s] = mean_of(row_of(pri_recv, table[0, s]), g)[0]

    parcels[segs] = jnp.zeros(parcels.shape[1:], F32)
    iota = lax.broadcasted_iota(jnp.int32, (8, points), 0)
    lanes = lax.broadcasted_iota(jnp.int32, (1, points), 1)
    steps = segs // total // GROUP
    for c in range(chunks):
        nodes = sec_recv[c]
        wait_recv(sec_send[c], nodes, 2 + c)

        @pl.loop(firsts[c] * steps, (firsts[c] + PHASES[c]) * steps)
        def _(i):
            group_values(nodes, lambda g: table[2, i * GROUP + g], lambda g: table[1, i * GROUP + g])
            for g in range(GROUP):
                s = table[1, i * GROUP + g]
                mean, inv = mean_of(row_of(nodes, table[2, i * GROUP + g]), g)
                w = jnp.where(lanes < counts[s], weights[pl.ds(s, 1), :], 0.0)
                diff = (mean - means[s]) * (w * inv)
                top = rounded(diff)
                gap_s[g] = jnp.where(iota < 4, top, diff - top)
            for g in range(GROUP):
                y = lax.dot_general(
                    gap_s[g].astype(BF16), both_s[g], (((1,), (1,)), ((), ())),
                    preferred_element_type=F32,
                )
                y = y[:, :n] + y[:, n:]
                parcels[i * GROUP + g] = y + pltpu.roll(y, 4, 0)

        def lift(p, dst):
            base = firsts[c] * quarter * devices + p * caps[c]
            for j in range(caps[c]):
                k = table[3, base + j]
                for d in range(3):
                    dst[p, d, j : j + 1, :] = parcels[k, d : d + 1, :]

        fill_and_start(lift, par_send[c], par_recv[c], 2 + chunks + c)

    wait_send(req_send, req_recv, 0)
    wait_send(pri_send, pri_recv, 1)
    for c in range(chunks):
        wait_send(sec_send[c], sec_recv[c], 2 + c)
    for c in range(chunks):
        wait_recv(par_send[c], par_recv[c], 2 + chunks + c)
        size = devices * caps[c]
        row = lax.broadcasted_iota(jnp.int32, (blocks, size), 0).astype(F32)
        select = jnp.where(row == hot[c : c + 1, :size], 1.0, 0.0).astype(BF16)
        for d in range(3):
            x = par_recv[c][:, d].reshape(size, n)
            top, mid, low = split_three(x)
            parts = jnp.concatenate([top, mid, low], axis=1).astype(BF16)
            y = jnp.dot(select, parts, preferred_element_type=F32)
            y = y[:, :n] + (y[:, n : 2 * n] + y[:, 2 * n :])
            gap[d] = y if c == 0 else gap[d] + y
    for c in range(chunks):
        wait_send(par_send[c], par_recv[c], 2 + chunks + c)


def body(node_coords, node_disp, qpoints, qweights, qcount, sec_block, pri_block):
    devices = lax.axis_size("gx") * lax.axis_size("gy")
    blocks, comps, n = node_coords.shape
    segs, _, points = qpoints.shape
    cap = 2 * segs // devices
    width = 2 * comps * n
    caps = [m * cap // sum(PHASES) for m in PHASES]
    kinds = 2 + 2 * len(caps)
    vmem, smem = pl.BlockSpec(memory_space=pltpu.VMEM), pl.BlockSpec(memory_space=pltpu.SMEM)
    gap = pl.pallas_call(
        fused_kernel,
        out_shape=jax.ShapeDtypeStruct((comps, blocks, n), F32),
        in_specs=[vmem, vmem, smem, vmem, vmem, vmem, vmem],
        out_specs=vmem,
        scratch_shapes=[
            pltpu.VMEM((devices, 1, 128), jnp.int32),
            pltpu.VMEM((devices, 1, 128), jnp.int32),
            pltpu.VMEM((devices, 128), F32),
            pltpu.SMEM((devices, 1, 128), jnp.int32),
            pltpu.VMEM((4, devices * cap), jnp.int32),
            pltpu.SMEM((4, devices * cap), jnp.int32),
            pltpu.VMEM((len(caps), devices * max(caps)), F32),
            pltpu.VMEM((devices, cap, width), F32),
            pltpu.VMEM((devices, cap, width), F32),
            pltpu.VMEM((segs, 8, points), F32),
            pltpu.VMEM((segs + 1, 8, n), F32),
            pltpu.VMEM((GROUP, 2 * n, points), BF16),
            pltpu.VMEM((GROUP, 8, points), F32),
            *[pltpu.VMEM((devices, m, width), F32) for m in caps + caps],
            *[pltpu.VMEM((devices, comps, m, n), F32) for m in caps + caps],
            pltpu.SemaphoreType.DMA((kinds, devices)),
            pltpu.SemaphoreType.DMA((kinds, devices)),
            pltpu.SemaphoreType.DMA((2,)),
        ],
        compiler_params=pltpu.CompilerParams(collective_id=0, has_side_effects=True),
        name="fused",
    )(
        pri_block, sec_block, qcount,
        node_coords.transpose(1, 0, 2), node_disp.transpose(1, 0, 2),
        qpoints.transpose(1, 0, 2), qweights,
    )
    return gap.transpose(1, 0, 2)


def solution(mesh):
    placed = (
        P(("gx", "gy"), None, None),
        P(("gx", "gy"), None, None),
        P(("gx", "gy"), None, None),
        P(("gx", "gy"), None),
        P(("gx", "gy")),
        P(("gx", "gy")),
        P(("gx", "gy")),
    )
    return jax.shard_map(
        body, mesh=mesh, in_specs=placed, out_specs=P(("gx", "gy"), None, None), check_vma=False
    )
```

```python
import functools
import jax
import jax.numpy as jnp
from jax import lax
from jax.experimental import pallas as pl
from jax.experimental.pallas import tpu as pltpu
from jax.sharding import PartitionSpec as P

GROUP = 16
PHASES = (2, 1, 1)
F32, BF16 = jnp.float32, jnp.bfloat16
MESH = pl.DeviceIdType.MESH


def rounded(x):
    return x.astype(BF16).astype(F32)


def stack_rows(rows, iota):
    out = jnp.zeros(iota.shape, F32)
    for i, row in rows:
        out = jnp.where(iota == i, row, out)
    return out


def disp_rows(row, n):
    iota = lax.broadcasted_iota(jnp.int32, (8, n), 0)
    u = [row[:, (3 + c) * n : (4 + c) * n] for c in range(3)]
    full = stack_rows([(i + 4 * h, u[i]) for h in range(2) for i in range(3)], iota)
    full = jnp.where((iota == 3) | (iota == 7), 1.0, full)
    both = jnp.where(iota < 4, rounded(full), full - rounded(full)).astype(BF16)
    return jnp.concatenate([both, both], axis=1)


def split_three(full):
    high = rounded(full)
    rest = full - high
    mid = rounded(rest)
    return high, mid, rest - mid


def point_features(qp, s):
    iota = lax.broadcasted_iota(jnp.int32, (8, qp.shape[2]), 0)
    x = [qp[c, pl.ds(s, 1), :] for c in range(3)]
    square = 1.0 + 2.0 * (x[0] * x[0] + x[1] * x[1] + x[2] * x[2])
    full = stack_rows([(0, x[0]), (1, x[1]), (2, x[2]), (3, 1.0), (4, square)], iota)
    high, mid, low = split_three(full)
    return jnp.concatenate([high, mid, high, low, high, mid], axis=0).astype(BF16)


def kernel_values(row, feat, n):
    iota = lax.broadcasted_iota(jnp.int32, (8, n), 0)
    x = [row[:, c * n : (c + 1) * n] for c in range(3)]
    square = 2.0 * (x[0] * x[0] + x[1] * x[1] + x[2] * x[2])
    full = stack_rows(
        [(0, -4.0 * x[0]), (1, -4.0 * x[1]), (2, -4.0 * x[2]), (3, square), (4, 1.0)], iota
    )
    high, mid, low = split_three(full)
    left = jnp.concatenate([high, high, mid, high, low, mid], axis=0)
    kern = 1.0 / jnp.dot(left.T.astype(BF16), feat, preferred_element_type=F32)
    kh = kern.astype(BF16)
    return kh, (kern - kh.astype(F32)).astype(BF16)


def floor_div(x, m):
    return jnp.floor((x + 0.5) * (1.0 / m))


def whole(x, size):
    return jnp.clip(x.astype(jnp.int32), 0, size - 1)


def one_hot_sum(lhs, match):
    return lax.dot_general(
        lhs.astype(BF16), jnp.where(match, 1.0, 0.0).astype(BF16), (((1,), (1,)), ((), ())),
        preferred_element_type=F32,
    )


def sixteens(x):
    high = jnp.floor(x * 0.0625)
    return high, x - 16.0 * high


def owners_of(block, blocks, cap):
    segs = block.shape[1]
    owner = floor_div(block, blocks)
    across = jnp.broadcast_to(owner, (segs, segs))
    down = across.T
    before = lax.broadcasted_iota(jnp.int32, (segs, segs), 0) < lax.broadcasted_iota(
        jnp.int32, (segs, segs), 1
    )
    same = jnp.where((down == across) & before, 1.0, 0.0)
    rank = jnp.sum(same, axis=0, keepdims=True)
    start = jnp.sum(jnp.where(down < across, 1.0, 0.0), axis=0, keepdims=True)
    return owner, block - owner * blocks, rank, start


def deal(owner, rank, start, segs, devices, cap):
    total = sum(PHASES)
    quarter = cap // total
    position = start + rank
    phase = position - total * floor_div(position, total)
    turn = place = slot = lane = jnp.zeros_like(owner)
    first = 0
    for count in PHASES:

        def before(x):
            turns = floor_div(x, total)
            return turns * count + jnp.clip(x - total * turns - first, 0.0, count)

        inside = (phase >= first) & (phase < first + count)
        spot = before(position)
        nth = spot - before(start)
        here = owner * (count * quarter) + nth
        turn = jnp.where(inside, spot + first * (segs // total), turn)
        slot = jnp.where(inside, here, slot)
        place = jnp.where(inside, here + first * quarter * devices, place)
        lane = jnp.where(inside, nth + (cap + first * quarter), lane)
        first += count
    return turn, slot, place, lane


def fused_kernel(
    pri_block, sec_block, counts, coords, disp, qp, weights, gap,
    req_send, req_recv, req_rows, ids, table_v, table, hot,
    pri_send, pri_recv, means, parcels, both_s, gap_s, *rest,
):
    chunks = len(PHASES)
    sec_send, rest = rest[:chunks], rest[chunks:]
    sec_recv, rest = rest[:chunks], rest[chunks:]
    par_send, rest = rest[:chunks], rest[chunks:]
    par_recv, rest = rest[:chunks], rest[chunks:]
    send_sem, recv_sem, local_sem = rest
    ny = lax.axis_size("gy")
    devices, cap, width = pri_send.shape
    n = width // 6
    segs, points = weights.shape
    blocks = coords.shape[1]
    slots = devices * cap
    total = sum(PHASES)
    quarter = cap // total
    firsts = [sum(PHASES[:c]) for c in range(chunks)]
    caps = [m * quarter for m in PHASES]
    nx = lax.axis_size("gx")
    gx, gy = lax.axis_index("gx"), lax.axis_index("gy")
    me = gx * ny + gy

    def device(t):
        far = lax.div(t, ny)
        if nx & (nx - 1):
            row = lax.rem(gx + far, nx)
        else:
            row, bit = 0, 1
            while bit < nx:
                row = row + bit * lax.rem(lax.div(gx, bit) + lax.div(far, bit), 2)
                bit *= 2
        return row, lax.rem(gy + t, ny)

    def partner(t):
        row, column = device(t)
        return row * ny + column

    def copy(src, dst, k, t):
        row, column = device(t)
        return pltpu.make_async_remote_copy(
            src_ref=src.at[row * ny + column],
            dst_ref=dst.at[me],
            send_sem=send_sem.at[k, t],
            recv_sem=recv_sem.at[k, t],
            device_id=(row, column),
            device_id_type=MESH,
        )

    def far_first(i):
        return devices - 1 - i

    def fill_and_start(fill, src, dst, k):
        fill(partner(far_first(0)), src)

        @pl.loop(1, devices - 1)
        def _(i):
            fill(partner(far_first(i)), src)
            copy(src, dst, k, far_first(i - 1)).start()

        fill(me, dst)
        copy(src, dst, k, far_first(devices - 2)).start()

    def fill_all(fill, src, dst):
        @pl.loop(1, devices)
        def _(t):
            fill(partner(t), src)

        fill(me, dst)

    def start_all(src, dst, k):
        @pl.loop(0, devices - 1)
        def _(i):
            copy(src, dst, k, far_first(i)).start()

    def wait_recv(src, dst, k):
        @pl.loop(1, devices)
        def _(t):
            copy(src, dst, k, t).wait_recv()

    def wait_send(src, dst, k):
        @pl.loop(1, devices)
        def _(t):
            copy(src, dst, k, t).wait_send()

    barrier = pltpu.get_barrier_semaphore()

    @pl.loop(1, devices)
    def _(t):
        pl.semaphore_signal(barrier, inc=1, device_id=device(t), device_id_type=MESH)

    pri = pri_block[...].reshape(1, segs).astype(F32)
    sec = sec_block[...].reshape(1, segs).astype(F32)
    pri_owner, pri_local, pri_rank, _ = owners_of(pri, blocks, cap)
    sec_owner, sec_local, sec_rank, sec_start = owners_of(sec, blocks, cap)
    turn, slot, place, lane = deal(sec_owner, sec_rank, sec_start, segs, devices, cap)
    owner = jnp.concatenate([pri_owner, sec_owner], axis=1)
    column = jnp.concatenate([pri_rank, lane], axis=1)
    local = jnp.concatenate([pri_local, sec_local], axis=1)
    to_owner = lax.broadcasted_iota(jnp.int32, (devices, 2 * segs), 0).astype(F32) == owner
    to_owner = jnp.where(to_owner, 1.0, 0.0)
    at_lane = lax.broadcasted_iota(jnp.int32, (128, 2 * segs), 0).astype(F32) == column
    pieces = [
        lax.dot_general(
            to_owner.astype(BF16), jnp.where(at_lane, part, 0.0).astype(BF16),
            (((1,), (1,)), ((), ())), preferred_element_type=F32,
        )
        for part in sixteens(local)
    ]
    req_rows[...] = 16.0 * pieces[0] + pieces[1]

    @pl.loop(0, devices)
    def _(p):
        req_send[p] = whole(req_rows[pl.ds(p, 1), :], blocks)

    req_recv[me] = whole(req_rows[pl.ds(me, 1), :], blocks)
    pl.semaphore_wait(barrier, devices - 1)

    start_all(req_send, req_recv, 0)

    number = lax.broadcasted_iota(jnp.int32, (1, segs), 1).astype(F32)
    zero = jnp.zeros((4, segs), F32)
    rows = jnp.concatenate([*sixteens(number), *sixteens(slot), zero], axis=0)
    match = lax.broadcasted_iota(jnp.int32, (segs, segs), 0).astype(F32) == turn
    found = one_hot_sum(rows, match)
    rows = jnp.concatenate([*sixteens(turn + 1.0), zero, zero[:2]], axis=0)
    match = lax.broadcasted_iota(jnp.int32, (slots, segs), 0).astype(F32) == place
    inverse = one_hot_sum(rows, match)
    inverse = 16.0 * inverse[0:1] + inverse[1:2] - 1.0
    inverse = jnp.where(inverse < 0.0, float(segs), inverse)
    turns = lax.broadcasted_iota(jnp.int32, (1, segs), 1)
    sizes = jnp.zeros_like(turns)
    for c in range(chunks):
        sizes = jnp.where(turns >= firsts[c] * (segs // total), devices * caps[c], sizes)
    table_v[0:1, :segs] = whole(pri_owner * cap + pri_rank, slots)
    table_v[1:2, :segs] = whole(16.0 * found[0:1] + found[1:2], segs)
    table_v[2:3, :segs] = whole(16.0 * found[2:3] + found[3:4], sizes)
    table_v[3:4, :] = whole(inverse, segs + 1)
    load_table = pltpu.make_async_copy(table_v, table, local_sem.at[0])
    load_table.start()

    wait_recv(req_send, req_recv, 0)
    load_ids = pltpu.make_async_copy(req_recv, ids, local_sem.at[1])
    load_ids.start()
    load_table.wait()
    load_ids.wait()

    def gather(base, count, p, dst):
        for j in range(count):
            b = ids[p, 0, base + j]
            for c in range(3):
                dst[p, j : j + 1, c * n : (c + 1) * n] = coords[c, pl.ds(b, 1), :]
                k = 3 + c
                dst[p, j : j + 1, k * n : (k + 1) * n] = disp[c, pl.ds(b, 1), :]

    fill_and_start(functools.partial(gather, 0, cap), pri_send, pri_recv, 1)
    for c in range(chunks):
        fill = functools.partial(gather, cap + firsts[c] * quarter, caps[c])
        fill_all(fill, sec_send[c], sec_recv[c])

    @pl.loop(0, devices)
    def _(p):
        req_rows[pl.ds(p, 1), :] = req_recv[p].astype(F32)

    high, low = sixteens(req_rows[...])
    for c in range(chunks):
        size = devices * caps[c]
        k = lax.broadcasted_iota(jnp.int32, (1, size), 1).astype(F32)
        from_row = floor_div(k, caps[c])
        from_lane = k - from_row * caps[c] + float(cap + firsts[c] * quarter)
        spread = lax.broadcasted_iota(jnp.int32, (128, size), 0).astype(F32) == from_lane
        spread = jnp.where(spread, 1.0, 0.0).astype(BF16)
        y = 16.0 * jnp.dot(high.astype(BF16), spread, preferred_element_type=F32)
        y = y + jnp.dot(low.astype(BF16), spread, preferred_element_type=F32)
        mine = lax.broadcasted_iota(jnp.int32, (devices, size), 0).astype(F32) == from_row
        hot[c : c + 1, :size] = jnp.sum(jnp.where(mine, y, 0.0), axis=0, keepdims=True)

    def row_of(nodes, spot):
        return nodes[spot // nodes.shape[1], pl.ds(lax.rem(spot, nodes.shape[1]), 1), :]

    def group_values(nodes, slot_of, seg_of):
        for g in range(GROUP):
            kh, kl = kernel_values(row_of(nodes, slot_of(g)), point_features(qp, seg_of(g)), n)
            both_s[g, :n] = kh
            both_s[g, n:] = kl

    def mean_of(row, g):
        a = jnp.dot(disp_rows(row, n), both_s[g], preferred_element_type=F32)
        sums = a + pltpu.roll(a, 4, 0)
        inv = 1.0 / sums[3:4]
        return sums * inv, inv

    wait_recv(pri_send, pri_recv, 1)
    start_all(sec_send[0], sec_recv[0], 2)

    @pl.loop(0, segs // GROUP)
    def _(i):
        group_values(pri_recv, lambda g: table[0, i * GROUP + g], lambda g: i * GROUP + g)
        for g in range(GROUP):
            s = i * GROUP + g
            means[s] = mean_of(row_of(pri_recv, table[0, s]), g)[0]

    parcels[segs] = jnp.zeros(parcels.shape[1:], F32)
    iota = lax.broadcasted_iota(jnp.int32, (8, points), 0)
    lanes = lax.broadcasted_iota(jnp.int32, (1, points), 1)
    steps = segs // total // GROUP
    for c in range(chunks):
        nodes = sec_recv[c]
        if c == 0:
            wait_send(req_send, req_recv, 0)
            wait_send(pri_send, pri_recv, 1)
        wait_recv(sec_send[c], nodes, 2 + c)
        if c == 0:
            for later in range(1, chunks):
                start_all(sec_send[later], sec_recv[later], 2 + later)

        @pl.loop(firsts[c] * steps, (firsts[c] + PHASES[c]) * steps)
        def _(i):
            group_values(nodes, lambda g: table[2, i * GROUP + g], lambda g: table[1, i * GROUP + g])
            for g in range(GROUP):
                s = table[1, i * GROUP + g]
                mean, inv = mean_of(row_of(nodes, table[2, i * GROUP + g]), g)
                w = jnp.where(lanes < counts[s], weights[pl.ds(s, 1), :], 0.0)
                diff = (mean - means[s]) * (w * inv)
                top = rounded(diff)
                gap_s[g] = jnp.where(iota < 4, top, diff - top)
            for g in range(GROUP):
                y = lax.dot_general(
                    gap_s[g].astype(BF16), both_s[g], (((1,), (1,)), ((), ())),
                    preferred_element_type=F32,
                )
                y = y[:, :n] + y[:, n:]
                parcels[i * GROUP + g] = y + pltpu.roll(y, 4, 0)

        def lift(p, dst):
            base = firsts[c] * quarter * devices + p * caps[c]
            for j in range(caps[c]):
                k = table[3, base + j]
                for d in range(3):
                    dst[p, d, j : j + 1, :] = parcels[k, d : d + 1, :]

        fill_and_start(lift, par_send[c], par_recv[c], 2 + chunks + c)

    for c in range(chunks):
        if c == chunks - 1:
            for k in range(chunks):
                wait_send(sec_send[k], sec_recv[k], 2 + k)
            for k in range(chunks - 1):
                wait_send(par_send[k], par_recv[k], 2 + chunks + k)
        wait_recv(par_send[c], par_recv[c], 2 + chunks + c)
        size = devices * caps[c]
        row = lax.broadcasted_iota(jnp.int32, (blocks, size), 0).astype(F32)
        select = jnp.where(row == hot[c : c + 1, :size], 1.0, 0.0).astype(BF16)
        for d in range(3):
            x = par_recv[c][:, d].reshape(size, n)
            top, mid, low = split_three(x)
            parts = jnp.concatenate([top, mid, low], axis=1).astype(BF16)
            y = jnp.dot(select, parts, preferred_element_type=F32)
            y = y[:, :n] + (y[:, n : 2 * n] + y[:, 2 * n :])
            gap[d] = y if c == 0 else gap[d] + y
    wait_send(par_send[-1], par_recv[-1], 1 + 2 * chunks)


def body(node_coords, node_disp, qpoints, qweights, qcount, sec_block, pri_block):
    devices = lax.axis_size("gx") * lax.axis_size("gy")
    blocks, comps, n = node_coords.shape
    segs, _, points = qpoints.shape
    cap = 2 * segs // devices
    width = 2 * comps * n
    caps = [m * cap // sum(PHASES) for m in PHASES]
    kinds = 2 + 2 * len(caps)
    vmem, smem = pl.BlockSpec(memory_space=pltpu.VMEM), pl.BlockSpec(memory_space=pltpu.SMEM)
    gap = pl.pallas_call(
        fused_kernel,
        out_shape=jax.ShapeDtypeStruct((comps, blocks, n), F32),
        in_specs=[vmem, vmem, smem, vmem, vmem, vmem, vmem],
        out_specs=vmem,
        scratch_shapes=[
            pltpu.VMEM((devices, 1, 128), jnp.int32),
            pltpu.VMEM((devices, 1, 128), jnp.int32),
            pltpu.VMEM((devices, 128), F32),
            pltpu.SMEM((devices, 1, 128), jnp.int32),
            pltpu.VMEM((4, devices * cap), jnp.int32),
            pltpu.SMEM((4, devices * cap), jnp.int32),
            pltpu.VMEM((len(caps), devices * max(caps)), F32),
            pltpu.VMEM((devices, cap, width), F32),
            pltpu.VMEM((devices, cap, width), F32),
            pltpu.VMEM((segs, 8, points), F32),
            pltpu.VMEM((segs + 1, 8, n), F32),
            pltpu.VMEM((GROUP, 2 * n, points), BF16),
            pltpu.VMEM((GROUP, 8, points), F32),
            *[pltpu.VMEM((devices, m, width), F32) for m in caps + caps],
            *[pltpu.VMEM((devices, comps, m, n), F32) for m in caps + caps],
            pltpu.SemaphoreType.DMA((kinds, devices)),
            pltpu.SemaphoreType.DMA((kinds, devices)),
            pltpu.SemaphoreType.DMA((2,)),
        ],
        compiler_params=pltpu.CompilerParams(collective_id=0, has_side_effects=True),
        name="fused",
    )(
        pri_block, sec_block, qcount,
        node_coords.transpose(1, 0, 2), node_disp.transpose(1, 0, 2),
        qpoints.transpose(1, 0, 2), qweights,
    )
    return gap.transpose(1, 0, 2)


def solution(mesh):
    placed = (
        P(("gx", "gy"), None, None),
        P(("gx", "gy"), None, None),
        P(("gx", "gy"), None, None),
        P(("gx", "gy"), None),
        P(("gx", "gy")),
        P(("gx", "gy")),
        P(("gx", "gy")),
    )
    return jax.shard_map(
        body, mesh=mesh, in_specs=placed, out_specs=P(("gx", "gy"), None, None), check_vma=False
    )
```

```python
import functools
import jax
import jax.numpy as jnp
from jax import lax
from jax.experimental import pallas as pl
from jax.experimental.pallas import tpu as pltpu
from jax.sharding import PartitionSpec as P

GROUP = 16
PHASES = (2, 1, 1)
F32, BF16 = jnp.float32, jnp.bfloat16
MESH = pl.DeviceIdType.MESH


def rounded(x):
    return x.astype(BF16).astype(F32)


def stack_rows(rows, iota):
    out = jnp.zeros(iota.shape, F32)
    for i, row in rows:
        out = jnp.where(iota == i, row, out)
    return out


def disp_rows(row, n):
    iota = lax.broadcasted_iota(jnp.int32, (8, n), 0)
    u = [row[:, (3 + c) * n : (4 + c) * n] for c in range(3)]
    full = stack_rows([(i + 4 * h, u[i]) for h in range(2) for i in range(3)], iota)
    full = jnp.where((iota == 3) | (iota == 7), 1.0, full)
    both = jnp.where(iota < 4, rounded(full), full - rounded(full)).astype(BF16)
    return jnp.concatenate([both, both], axis=1)


def split_three(full):
    high = rounded(full)
    rest = full - high
    mid = rounded(rest)
    return high, mid, rest - mid


def point_features(qp, s):
    iota = lax.broadcasted_iota(jnp.int32, (8, qp.shape[2]), 0)
    x = [qp[c, pl.ds(s, 1), :] for c in range(3)]
    square = 1.0 + 2.0 * (x[0] * x[0] + x[1] * x[1] + x[2] * x[2])
    full = stack_rows([(0, x[0]), (1, x[1]), (2, x[2]), (3, 1.0), (4, square)], iota)
    high, mid, low = split_three(full)
    return jnp.concatenate([high, mid, high, low, high, mid], axis=0).astype(BF16)


def kernel_values(row, feat, n):
    iota = lax.broadcasted_iota(jnp.int32, (8, n), 0)
    x = [row[:, c * n : (c + 1) * n] for c in range(3)]
    square = 2.0 * (x[0] * x[0] + x[1] * x[1] + x[2] * x[2])
    full = stack_rows(
        [(0, -4.0 * x[0]), (1, -4.0 * x[1]), (2, -4.0 * x[2]), (3, square), (4, 1.0)], iota
    )
    high, mid, low = split_three(full)
    left = jnp.concatenate([high, high, mid, high, low, mid], axis=0)
    kern = 1.0 / jnp.dot(left.T.astype(BF16), feat, preferred_element_type=F32)
    kh = kern.astype(BF16)
    return kh, (kern - kh.astype(F32)).astype(BF16)


def floor_div(x, m):
    return jnp.floor((x + 0.5) * (1.0 / m))


def whole(x, size):
    return jnp.clip(x.astype(jnp.int32), 0, size - 1)


def one_hot_sum(lhs, match):
    return lax.dot_general(
        lhs.astype(BF16), jnp.where(match, 1.0, 0.0).astype(BF16), (((1,), (1,)), ((), ())),
        preferred_element_type=F32,
    )


def sixteens(x):
    high = jnp.floor(x * 0.0625)
    return high, x - 16.0 * high


def owners_of(block, blocks, cap):
    segs = block.shape[1]
    owner = floor_div(block, blocks)
    across = jnp.broadcast_to(owner, (segs, segs))
    down = across.T
    before = lax.broadcasted_iota(jnp.int32, (segs, segs), 0) < lax.broadcasted_iota(
        jnp.int32, (segs, segs), 1
    )
    same = jnp.where((down == across) & before, 1.0, 0.0)
    rank = jnp.sum(same, axis=0, keepdims=True)
    start = jnp.sum(jnp.where(down < across, 1.0, 0.0), axis=0, keepdims=True)
    return owner, block - owner * blocks, rank, start


def deal(owner, rank, start, segs, devices, cap):
    total = sum(PHASES)
    quarter = cap // total
    position = start + rank
    phase = position - total * floor_div(position, total)
    turn = place = slot = lane = jnp.zeros_like(owner)
    first = 0
    for count in PHASES:

        def before(x):
            turns = floor_div(x, total)
            return turns * count + jnp.clip(x - total * turns - first, 0.0, count)

        inside = (phase >= first) & (phase < first + count)
        spot = before(position)
        nth = spot - before(start)
        here = owner * (count * quarter) + nth
        turn = jnp.where(inside, spot + first * (segs // total), turn)
        slot = jnp.where(inside, here, slot)
        place = jnp.where(inside, here + first * quarter * devices, place)
        lane = jnp.where(inside, nth + (cap + first * quarter), lane)
        first += count
    return turn, slot, place, lane


def fused_kernel(
    pri_block, sec_block, counts, coords_h, disp_h, qp_h, weights_h, gap,
    coords, disp, qp, weights, req_send, req_recv, req_rows, ids, table_v, table, hot,
    pri_send, pri_recv, means, parcels, both_s, gap_s, *rest,
):
    chunks = len(PHASES)
    sec_send, rest = rest[:chunks], rest[chunks:]
    sec_recv, rest = rest[:chunks], rest[chunks:]
    par_send, rest = rest[:chunks], rest[chunks:]
    par_recv, rest = rest[:chunks], rest[chunks:]
    send_sem, recv_sem, local_sem = rest
    ny = lax.axis_size("gy")
    devices, cap, width = pri_send.shape
    n = width // 6
    segs, points = weights.shape
    blocks = coords.shape[1]
    slots = devices * cap
    total = sum(PHASES)
    quarter = cap // total
    firsts = [sum(PHASES[:c]) for c in range(chunks)]
    caps = [m * quarter for m in PHASES]
    nx = lax.axis_size("gx")
    gx, gy = lax.axis_index("gx"), lax.axis_index("gy")
    me = gx * ny + gy

    def device(t):
        far = lax.div(t, ny)
        if nx & (nx - 1):
            row = lax.rem(gx + far, nx)
        else:
            row, bit = 0, 1
            while bit < nx:
                row = row + bit * lax.rem(lax.div(gx, bit) + lax.div(far, bit), 2)
                bit *= 2
        return row, lax.rem(gy + t, ny)

    def partner(t):
        row, column = device(t)
        return row * ny + column

    def copy(src, dst, k, t):
        row, column = device(t)
        return pltpu.make_async_remote_copy(
            src_ref=src.at[row * ny + column],
            dst_ref=dst.at[me],
            send_sem=send_sem.at[k],
            recv_sem=recv_sem.at[k],
            device_id=(row, column),
            device_id_type=MESH,
        )

    def far_first(i):
        return devices - 1 - i

    def fill_and_start(fill, src, dst, k):
        fill(partner(far_first(0)), src)

        @pl.loop(1, devices - 1)
        def _(i):
            fill(partner(far_first(i)), src)
            copy(src, dst, k, far_first(i - 1)).start()

        fill(me, dst)
        copy(src, dst, k, far_first(devices - 2)).start()

    def fill_all(fill, src, dst):
        @pl.loop(1, devices)
        def _(t):
            fill(partner(t), src)

        fill(me, dst)

    def start_all(src, dst, k):
        @pl.loop(0, devices - 1)
        def _(i):
            copy(src, dst, k, far_first(i)).start()

    def all_of(src, dst, k):
        row, column = device(1)
        return pltpu.make_async_remote_copy(
            src_ref=src.at[pl.ds(0, devices - 1)],
            dst_ref=dst.at[pl.ds(0, devices - 1)],
            send_sem=send_sem.at[k],
            recv_sem=recv_sem.at[k],
            device_id=(row, column),
            device_id_type=MESH,
        )

    def wait_recv(src, dst, k):
        all_of(src, dst, k).wait_recv()

    def wait_send(src, dst, k):
        all_of(src, dst, k).wait_send()

    loads = [
        pltpu.make_async_copy(src, dst, local_sem.at[2 + i])
        for i, (src, dst) in enumerate(
            [(coords_h, coords), (disp_h, disp), (qp_h, qp), (weights_h, weights)]
        )
    ]
    for load in loads:
        load.start()
    barrier = pltpu.get_barrier_semaphore()

    @pl.loop(1, devices)
    def _(t):
        pl.semaphore_signal(barrier, inc=1, device_id=device(t), device_id_type=MESH)

    pri = pri_block[...].reshape(1, segs).astype(F32)
    sec = sec_block[...].reshape(1, segs).astype(F32)
    pri_owner, pri_local, pri_rank, _ = owners_of(pri, blocks, cap)
    sec_owner, sec_local, sec_rank, sec_start = owners_of(sec, blocks, cap)
    turn, slot, place, lane = deal(sec_owner, sec_rank, sec_start, segs, devices, cap)
    owner = jnp.concatenate([pri_owner, sec_owner], axis=1)
    column = jnp.concatenate([pri_rank, lane], axis=1)
    local = jnp.concatenate([pri_local, sec_local], axis=1)
    to_owner = lax.broadcasted_iota(jnp.int32, (devices, 2 * segs), 0).astype(F32) == owner
    to_owner = jnp.where(to_owner, 1.0, 0.0)
    at_lane = lax.broadcasted_iota(jnp.int32, (128, 2 * segs), 0).astype(F32) == column
    pieces = [
        lax.dot_general(
            to_owner.astype(BF16), jnp.where(at_lane, part, 0.0).astype(BF16),
            (((1,), (1,)), ((), ())), preferred_element_type=F32,
        )
        for part in sixteens(local)
    ]
    req_rows[...] = 16.0 * pieces[0] + pieces[1]

    @pl.loop(0, devices)
    def _(p):
        req_send[p] = whole(req_rows[pl.ds(p, 1), :], blocks)

    req_recv[me] = whole(req_rows[pl.ds(me, 1), :], blocks)
    pl.semaphore_wait(barrier, devices - 1)

    start_all(req_send, req_recv, 0)

    number = lax.broadcasted_iota(jnp.int32, (1, segs), 1).astype(F32)
    zero = jnp.zeros((4, segs), F32)
    rows = jnp.concatenate([*sixteens(number), *sixteens(slot), zero], axis=0)
    match = lax.broadcasted_iota(jnp.int32, (segs, segs), 0).astype(F32) == turn
    found = one_hot_sum(rows, match)
    rows = jnp.concatenate([*sixteens(turn + 1.0), zero, zero[:2]], axis=0)
    match = lax.broadcasted_iota(jnp.int32, (slots, segs), 0).astype(F32) == place
    inverse = one_hot_sum(rows, match)
    inverse = 16.0 * inverse[0:1] + inverse[1:2] - 1.0
    inverse = jnp.where(inverse < 0.0, float(segs), inverse)
    turns = lax.broadcasted_iota(jnp.int32, (1, segs), 1)
    sizes = jnp.zeros_like(turns)
    for c in range(chunks):
        sizes = jnp.where(turns >= firsts[c] * (segs // total), devices * caps[c], sizes)
    table_v[0:1, :segs] = whole(pri_owner * cap + pri_rank, slots)
    table_v[1:2, :segs] = whole(16.0 * found[0:1] + found[1:2], segs)
    table_v[2:3, :segs] = whole(16.0 * found[2:3] + found[3:4], sizes)
    table_v[3:4, :] = whole(inverse, segs + 1)
    load_table = pltpu.make_async_copy(table_v, table, local_sem.at[0])
    load_table.start()

    wait_recv(req_send, req_recv, 0)
    load_ids = pltpu.make_async_copy(req_recv, ids, local_sem.at[1])
    load_ids.start()
    for load in loads:
        load.wait()
    load_table.wait()
    load_ids.wait()

    def gather(base, count, p, dst):
        for j in range(count):
            b = ids[p, 0, base + j]
            for c in range(3):
                dst[p, j : j + 1, c * n : (c + 1) * n] = coords[c, pl.ds(b, 1), :]
                k = 3 + c
                dst[p, j : j + 1, k * n : (k + 1) * n] = disp[c, pl.ds(b, 1), :]

    fill_and_start(functools.partial(gather, 0, cap), pri_send, pri_recv, 1)
    for c in range(chunks):
        fill = functools.partial(gather, cap + firsts[c] * quarter, caps[c])
        fill_all(fill, sec_send[c], sec_recv[c])

    @pl.loop(0, devices)
    def _(p):
        req_rows[pl.ds(p, 1), :] = req_recv[p].astype(F32)

    high, low = sixteens(req_rows[...])
    for c in range(chunks):
        size = devices * caps[c]
        k = lax.broadcasted_iota(jnp.int32, (1, size), 1).astype(F32)
        from_row = floor_div(k, caps[c])
        from_lane = k - from_row * caps[c] + float(cap + firsts[c] * quarter)
        spread = lax.broadcasted_iota(jnp.int32, (128, size), 0).astype(F32) == from_lane
        spread = jnp.where(spread, 1.0, 0.0).astype(BF16)
        y = 16.0 * jnp.dot(high.astype(BF16), spread, preferred_element_type=F32)
        y = y + jnp.dot(low.astype(BF16), spread, preferred_element_type=F32)
        mine = lax.broadcasted_iota(jnp.int32, (devices, size), 0).astype(F32) == from_row
        hot[c : c + 1, :size] = jnp.sum(jnp.where(mine, y, 0.0), axis=0, keepdims=True)

    def row_of(nodes, spot):
        return nodes[spot // nodes.shape[1], pl.ds(lax.rem(spot, nodes.shape[1]), 1), :]

    def group_values(nodes, slot_of, seg_of):
        for g in range(GROUP):
            kh, kl = kernel_values(row_of(nodes, slot_of(g)), point_features(qp, seg_of(g)), n)
            both_s[g, :n] = kh
            both_s[g, n:] = kl

    def mean_of(row, g):
        a = jnp.dot(disp_rows(row, n), both_s[g], preferred_element_type=F32)
        sums = a + pltpu.roll(a, 4, 0)
        inv = 1.0 / sums[3:4]
        return sums * inv, inv

    wait_recv(pri_send, pri_recv, 1)
    start_all(sec_send[0], sec_recv[0], 2)

    @pl.loop(0, segs // GROUP)
    def _(i):
        group_values(pri_recv, lambda g: table[0, i * GROUP + g], lambda g: i * GROUP + g)
        for g in range(GROUP):
            s = i * GROUP + g
            means[s] = mean_of(row_of(pri_recv, table[0, s]), g)[0]

    parcels[segs] = jnp.zeros(parcels.shape[1:], F32)
    iota = lax.broadcasted_iota(jnp.int32, (8, points), 0)
    lanes = lax.broadcasted_iota(jnp.int32, (1, points), 1)
    steps = segs // total // GROUP
    for c in range(chunks):
        nodes = sec_recv[c]
        if c == 0:
            wait_send(req_send, req_recv, 0)
            wait_send(pri_send, pri_recv, 1)
        wait_recv(sec_send[c], nodes, 2 + c)
        if c == 0:
            for later in range(1, chunks):
                start_all(sec_send[later], sec_recv[later], 2 + later)

        @pl.loop(firsts[c] * steps, (firsts[c] + PHASES[c]) * steps)
        def _(i):
            group_values(nodes, lambda g: table[2, i * GROUP + g], lambda g: table[1, i * GROUP + g])
            for g in range(GROUP):
                s = table[1, i * GROUP + g]
                mean, inv = mean_of(row_of(nodes, table[2, i * GROUP + g]), g)
                w = jnp.where(lanes < counts[s], weights[pl.ds(s, 1), :], 0.0)
                diff = (mean - means[s]) * (w * inv)
                top = rounded(diff)
                gap_s[g] = jnp.where(iota < 4, top, diff - top)
            for g in range(GROUP):
                y = lax.dot_general(
                    gap_s[g].astype(BF16), both_s[g], (((1,), (1,)), ((), ())),
                    preferred_element_type=F32,
                )
                y = y[:, :n] + y[:, n:]
                parcels[i * GROUP + g] = y + pltpu.roll(y, 4, 0)

        def lift(p, dst):
            base = firsts[c] * quarter * devices + p * caps[c]
            for j in range(caps[c]):
                k = table[3, base + j]
                for d in range(3):
                    dst[p, d, j : j + 1, :] = parcels[k, d : d + 1, :]

        fill_and_start(lift, par_send[c], par_recv[c], 2 + chunks + c)

    for c in range(chunks):
        if c == chunks - 1:
            for k in range(chunks):
                wait_send(sec_send[k], sec_recv[k], 2 + k)
            for k in range(chunks - 1):
                wait_send(par_send[k], par_recv[k], 2 + chunks + k)
        wait_recv(par_send[c], par_recv[c], 2 + chunks + c)
        size = devices * caps[c]
        row = lax.broadcasted_iota(jnp.int32, (blocks, size), 0).astype(F32)
        select = jnp.where(row == hot[c : c + 1, :size], 1.0, 0.0).astype(BF16)
        for d in range(3):
            x = par_recv[c][:, d].reshape(size, n)
            top, mid, low = split_three(x)
            parts = jnp.concatenate([top, mid, low], axis=1).astype(BF16)
            y = jnp.dot(select, parts, preferred_element_type=F32)
            y = y[:, :n] + (y[:, n : 2 * n] + y[:, 2 * n :])
            gap[d] = y if c == 0 else gap[d] + y
    wait_send(par_send[-1], par_recv[-1], 1 + 2 * chunks)


def body(node_coords, node_disp, qpoints, qweights, qcount, sec_block, pri_block):
    devices = lax.axis_size("gx") * lax.axis_size("gy")
    blocks, comps, n = node_coords.shape
    segs, _, points = qpoints.shape
    cap = 2 * segs // devices
    width = 2 * comps * n
    caps = [m * cap // sum(PHASES) for m in PHASES]
    kinds = 2 + 2 * len(caps)
    vmem, smem = pl.BlockSpec(memory_space=pltpu.VMEM), pl.BlockSpec(memory_space=pltpu.SMEM)
    gap = pl.pallas_call(
        fused_kernel,
        out_shape=pltpu.VMEM((comps, blocks, n), F32),
        in_specs=[vmem, vmem, smem] + [pl.BlockSpec(memory_space=pltpu.HBM)] * 4,
        out_specs=vmem,
        scratch_shapes=[
            pltpu.VMEM((comps, blocks, n), F32),
            pltpu.VMEM((comps, blocks, n), F32),
            pltpu.VMEM((comps, segs, points), F32),
            pltpu.VMEM((segs, points), F32),
            pltpu.VMEM((devices, 1, 128), jnp.int32),
            pltpu.VMEM((devices, 1, 128), jnp.int32),
            pltpu.VMEM((devices, 128), F32),
            pltpu.SMEM((devices, 1, 128), jnp.int32),
            pltpu.VMEM((4, devices * cap), jnp.int32),
            pltpu.SMEM((4, devices * cap), jnp.int32),
            pltpu.VMEM((len(caps), devices * max(caps)), F32),
            pltpu.VMEM((devices, cap, width), F32),
            pltpu.VMEM((devices, cap, width), F32),
            pltpu.VMEM((segs, 8, points), F32),
            pltpu.VMEM((segs + 1, 8, n), F32),
            pltpu.VMEM((GROUP, 2 * n, points), BF16),
            pltpu.VMEM((GROUP, 8, points), F32),
            *[pltpu.VMEM((devices, m, width), F32) for m in caps + caps],
            *[pltpu.VMEM((devices, comps, m, n), F32) for m in caps + caps],
            pltpu.SemaphoreType.DMA((kinds,)),
            pltpu.SemaphoreType.DMA((kinds,)),
            pltpu.SemaphoreType.DMA((6,)),
        ],
        compiler_params=pltpu.CompilerParams(collective_id=0, has_side_effects=True),
        name="fused",
    )(
        pri_block, sec_block, qcount,
        node_coords.transpose(1, 0, 2), node_disp.transpose(1, 0, 2),
        qpoints.transpose(1, 0, 2), qweights,
    )
    return gap.transpose(1, 0, 2)


def solution(mesh):
    placed = (
        P(("gx", "gy"), None, None),
        P(("gx", "gy"), None, None),
        P(("gx", "gy"), None, None),
        P(("gx", "gy"), None),
        P(("gx", "gy")),
        P(("gx", "gy")),
        P(("gx", "gy")),
    )
    return jax.shard_map(
        body, mesh=mesh, in_specs=placed, out_specs=P(("gx", "gy"), None, None), check_vma=False
    )
```

```python
import functools
import jax
import jax.numpy as jnp
from jax import lax
from jax.experimental import pallas as pl
from jax.experimental.pallas import tpu as pltpu
from jax.sharding import PartitionSpec as P

GROUP = 16
PHASES = (2, 1, 1)
F32, BF16 = jnp.float32, jnp.bfloat16
MESH = pl.DeviceIdType.MESH


def rounded(x):
    return x.astype(BF16).astype(F32)


def stack_rows(rows, iota):
    out = jnp.zeros(iota.shape, F32)
    for i, row in rows:
        out = jnp.where(iota == i, row, out)
    return out


def disp_rows(row, n):
    iota = lax.broadcasted_iota(jnp.int32, (8, n), 0)
    u = [row[:, (3 + c) * n : (4 + c) * n] for c in range(3)]
    full = stack_rows([(i + 4 * h, u[i]) for h in range(2) for i in range(3)], iota)
    full = jnp.where((iota == 3) | (iota == 7), 1.0, full)
    both = jnp.where(iota < 4, rounded(full), full - rounded(full)).astype(BF16)
    return jnp.concatenate([both, both], axis=1)


def split_three(full):
    high = rounded(full)
    rest = full - high
    mid = rounded(rest)
    return high, mid, rest - mid


def point_features(qp, s):
    iota = lax.broadcasted_iota(jnp.int32, (8, qp.shape[2]), 0)
    x = [qp[c, pl.ds(s, 1), :] for c in range(3)]
    square = 1.0 + 2.0 * (x[0] * x[0] + x[1] * x[1] + x[2] * x[2])
    full = stack_rows([(0, x[0]), (1, x[1]), (2, x[2]), (3, 1.0), (4, square)], iota)
    high, mid, low = split_three(full)
    return jnp.concatenate([high, mid, high, low, high, mid], axis=0).astype(BF16)


def kernel_values(row, feat, n):
    iota = lax.broadcasted_iota(jnp.int32, (8, n), 0)
    x = [row[:, c * n : (c + 1) * n] for c in range(3)]
    square = 2.0 * (x[0] * x[0] + x[1] * x[1] + x[2] * x[2])
    full = stack_rows(
        [(0, -4.0 * x[0]), (1, -4.0 * x[1]), (2, -4.0 * x[2]), (3, square), (4, 1.0)], iota
    )
    high, mid, low = split_three(full)
    left = jnp.concatenate([high, high, mid, high, low, mid], axis=0)
    kern = 1.0 / jnp.dot(left.T.astype(BF16), feat, preferred_element_type=F32)
    kh = kern.astype(BF16)
    return kh, (kern - kh.astype(F32)).astype(BF16)


def floor_div(x, m):
    return jnp.floor((x + 0.5) * (1.0 / m))


def whole(x, size):
    return jnp.clip(x.astype(jnp.int32), 0, size - 1)


def one_hot_sum(lhs, match):
    return lax.dot_general(
        lhs.astype(BF16), jnp.where(match, 1.0, 0.0).astype(BF16), (((1,), (1,)), ((), ())),
        preferred_element_type=F32,
    )


def sixteens(x):
    high = jnp.floor(x * 0.0625)
    return high, x - 16.0 * high


def owners_of(block, blocks, cap):
    segs = block.shape[1]
    owner = floor_div(block, blocks)
    across = jnp.broadcast_to(owner, (segs, segs))
    down = across.T
    before = lax.broadcasted_iota(jnp.int32, (segs, segs), 0) < lax.broadcasted_iota(
        jnp.int32, (segs, segs), 1
    )
    same = jnp.where((down == across) & before, 1.0, 0.0)
    rank = jnp.sum(same, axis=0, keepdims=True)
    start = jnp.sum(jnp.where(down < across, 1.0, 0.0), axis=0, keepdims=True)
    return owner, block - owner * blocks, rank, start


def deal(owner, rank, start, segs, devices, cap):
    total = sum(PHASES)
    quarter = cap // total
    position = start + rank
    phase = position - total * floor_div(position, total)
    turn = place = slot = lane = jnp.zeros_like(owner)
    first = 0
    for count in PHASES:

        def before(x):
            turns = floor_div(x, total)
            return turns * count + jnp.clip(x - total * turns - first, 0.0, count)

        inside = (phase >= first) & (phase < first + count)
        spot = before(position)
        nth = spot - before(start)
        here = owner * (count * quarter) + nth
        turn = jnp.where(inside, spot + first * (segs // total), turn)
        slot = jnp.where(inside, here, slot)
        place = jnp.where(inside, here + first * quarter * devices, place)
        lane = jnp.where(inside, nth + (cap + first * quarter), lane)
        first += count
    return turn, slot, place, lane


def fused_kernel(
    pri_block, sec_block, counts, coords_h, disp_h, qp_h, weights_h, gap,
    coords, disp, qp, weights, feats, req_send, req_recv, req_rows, ids, table_v, table, hot,
    pri_send, pri_recv, means, parcels, both_s, gap_s, *rest,
):
    chunks = len(PHASES)
    sec_send, rest = rest[:chunks], rest[chunks:]
    sec_recv, rest = rest[:chunks], rest[chunks:]
    par_send, rest = rest[:chunks], rest[chunks:]
    par_recv, rest = rest[:chunks], rest[chunks:]
    send_sem, recv_sem, local_sem = rest
    ny = lax.axis_size("gy")
    devices, cap, width = pri_send.shape
    n = width // 6
    segs, points = weights.shape
    blocks = coords.shape[1]
    slots = devices * cap
    total = sum(PHASES)
    quarter = cap // total
    firsts = [sum(PHASES[:c]) for c in range(chunks)]
    caps = [m * quarter for m in PHASES]
    nx = lax.axis_size("gx")
    gx, gy = lax.axis_index("gx"), lax.axis_index("gy")
    me = gx * ny + gy

    def device(t):
        far = lax.div(t, ny)
        if nx & (nx - 1):
            row = lax.rem(gx + far, nx)
        else:
            row, bit = 0, 1
            while bit < nx:
                row = row + bit * lax.rem(lax.div(gx, bit) + lax.div(far, bit), 2)
                bit *= 2
        return row, lax.rem(gy + t, ny)

    def partner(t):
        row, column = device(t)
        return row * ny + column

    def copy(src, dst, k, t):
        row, column = device(t)
        return pltpu.make_async_remote_copy(
            src_ref=src.at[row * ny + column],
            dst_ref=dst.at[me],
            send_sem=send_sem.at[k],
            recv_sem=recv_sem.at[k],
            device_id=(row, column),
            device_id_type=MESH,
        )

    def far_first(i):
        return devices - 1 - i

    def fill_and_start(fill, src, dst, k):
        fill(partner(far_first(0)), src)

        @pl.loop(1, devices - 1)
        def _(i):
            fill(partner(far_first(i)), src)
            copy(src, dst, k, far_first(i - 1)).start()

        fill(me, dst)
        copy(src, dst, k, far_first(devices - 2)).start()

    def fill_all(fill, src, dst):
        @pl.loop(1, devices)
        def _(t):
            fill(partner(t), src)

        fill(me, dst)

    def start_all(src, dst, k):
        @pl.loop(0, devices - 1)
        def _(i):
            copy(src, dst, k, far_first(i)).start()

    def all_of(src, dst, k):
        row, column = device(1)
        return pltpu.make_async_remote_copy(
            src_ref=src.at[pl.ds(0, devices - 1)],
            dst_ref=dst.at[pl.ds(0, devices - 1)],
            send_sem=send_sem.at[k],
            recv_sem=recv_sem.at[k],
            device_id=(row, column),
            device_id_type=MESH,
        )

    def wait_recv(src, dst, k):
        all_of(src, dst, k).wait_recv()

    def wait_send(src, dst, k):
        all_of(src, dst, k).wait_send()

    loads = [
        pltpu.make_async_copy(src, dst, local_sem.at[2 + i])
        for i, (src, dst) in enumerate(
            [(coords_h, coords), (disp_h, disp), (qp_h, qp), (weights_h, weights)]
        )
    ]
    for load in loads:
        load.start()
    barrier = pltpu.get_barrier_semaphore()

    @pl.loop(0, devices - 1)
    def _(i):
        pl.semaphore_signal(
            barrier, inc=1, device_id=device(far_first(i)), device_id_type=MESH
        )

    pri = pri_block[...].reshape(1, segs).astype(F32)
    sec = sec_block[...].reshape(1, segs).astype(F32)
    pri_owner, pri_local, pri_rank, _ = owners_of(pri, blocks, cap)
    sec_owner, sec_local, sec_rank, sec_start = owners_of(sec, blocks, cap)
    turn, slot, place, lane = deal(sec_owner, sec_rank, sec_start, segs, devices, cap)
    owner = jnp.concatenate([pri_owner, sec_owner], axis=1)
    column = jnp.concatenate([pri_rank, lane], axis=1)
    local = jnp.concatenate([pri_local, sec_local], axis=1)
    to_owner = lax.broadcasted_iota(jnp.int32, (devices, 2 * segs), 0).astype(F32) == owner
    to_owner = jnp.where(to_owner, 1.0, 0.0)
    at_lane = lax.broadcasted_iota(jnp.int32, (128, 2 * segs), 0).astype(F32) == column
    pieces = [
        lax.dot_general(
            to_owner.astype(BF16), jnp.where(at_lane, part, 0.0).astype(BF16),
            (((1,), (1,)), ((), ())), preferred_element_type=F32,
        )
        for part in sixteens(local)
    ]
    req_rows[...] = 16.0 * pieces[0] + pieces[1]

    @pl.loop(0, devices)
    def _(p):
        req_send[p] = whole(req_rows[pl.ds(p, 1), :], blocks)

    req_recv[me] = whole(req_rows[pl.ds(me, 1), :], blocks)
    pl.semaphore_wait(barrier, devices - 1)

    start_all(req_send, req_recv, 0)

    number = lax.broadcasted_iota(jnp.int32, (1, segs), 1).astype(F32)
    zero = jnp.zeros((4, segs), F32)
    rows = jnp.concatenate([*sixteens(number), *sixteens(slot), zero], axis=0)
    match = lax.broadcasted_iota(jnp.int32, (segs, segs), 0).astype(F32) == turn
    found = one_hot_sum(rows, match)
    rows = jnp.concatenate([*sixteens(turn + 1.0), zero, zero[:2]], axis=0)
    match = lax.broadcasted_iota(jnp.int32, (slots, segs), 0).astype(F32) == place
    inverse = one_hot_sum(rows, match)
    inverse = 16.0 * inverse[0:1] + inverse[1:2] - 1.0
    inverse = jnp.where(inverse < 0.0, float(segs), inverse)
    turns = lax.broadcasted_iota(jnp.int32, (1, segs), 1)
    sizes = jnp.zeros_like(turns)
    for c in range(chunks):
        sizes = jnp.where(turns >= firsts[c] * (segs // total), devices * caps[c], sizes)
    table_v[0:1, :segs] = whole(pri_owner * cap + pri_rank, slots)
    table_v[1:2, :segs] = whole(16.0 * found[0:1] + found[1:2], segs)
    table_v[2:3, :segs] = whole(16.0 * found[2:3] + found[3:4], sizes)
    table_v[3:4, :] = whole(inverse, segs + 1)
    load_table = pltpu.make_async_copy(table_v, table, local_sem.at[0])
    load_table.start()

    wait_recv(req_send, req_recv, 0)
    load_ids = pltpu.make_async_copy(req_recv, ids, local_sem.at[1])
    load_ids.start()
    for load in loads:
        load.wait()
    load_table.wait()
    load_ids.wait()

    def gather(base, count, p, dst):
        for j in range(count):
            b = ids[p, 0, base + j]
            for c in range(3):
                dst[p, j : j + 1, c * n : (c + 1) * n] = coords[c, pl.ds(b, 1), :]
                k = 3 + c
                dst[p, j : j + 1, k * n : (k + 1) * n] = disp[c, pl.ds(b, 1), :]

    fill_and_start(functools.partial(gather, 0, cap), pri_send, pri_recv, 1)
    for c in range(chunks):
        fill = functools.partial(gather, cap + firsts[c] * quarter, caps[c])
        fill_all(fill, sec_send[c], sec_recv[c])

    @pl.loop(0, devices)
    def _(p):
        req_rows[pl.ds(p, 1), :] = req_recv[p].astype(F32)

    high, low = sixteens(req_rows[...])
    for c in range(chunks):
        size = devices * caps[c]
        k = lax.broadcasted_iota(jnp.int32, (1, size), 1).astype(F32)
        from_row = floor_div(k, caps[c])
        from_lane = k - from_row * caps[c] + float(cap + firsts[c] * quarter)
        spread = lax.broadcasted_iota(jnp.int32, (128, size), 0).astype(F32) == from_lane
        spread = jnp.where(spread, 1.0, 0.0).astype(BF16)
        y = 16.0 * jnp.dot(high.astype(BF16), spread, preferred_element_type=F32)
        y = y + jnp.dot(low.astype(BF16), spread, preferred_element_type=F32)
        mine = lax.broadcasted_iota(jnp.int32, (devices, size), 0).astype(F32) == from_row
        hot[c : c + 1, :size] = jnp.sum(jnp.where(mine, y, 0.0), axis=0, keepdims=True)

    def row_of(nodes, spot):
        return nodes[spot // nodes.shape[1], pl.ds(lax.rem(spot, nodes.shape[1]), 1), :]

    def group_values(nodes, slot_of, feat_of):
        for g in range(GROUP):
            kh, kl = kernel_values(row_of(nodes, slot_of(g)), feat_of(g), n)
            both_s[g, :n] = kh
            both_s[g, n:] = kl

    def mean_of(row, g):
        a = jnp.dot(disp_rows(row, n), both_s[g], preferred_element_type=F32)
        sums = a + pltpu.roll(a, 4, 0)
        inv = 1.0 / sums[3:4]
        return sums * inv, inv

    wait_recv(pri_send, pri_recv, 1)
    start_all(sec_send[0], sec_recv[0], 2)

    @pl.loop(0, segs // GROUP)
    def _(i):
        def fresh(g):
            feat = point_features(qp, i * GROUP + g)
            feats[i * GROUP + g] = feat
            return feat

        group_values(pri_recv, lambda g: table[0, i * GROUP + g], fresh)
        for g in range(GROUP):
            s = i * GROUP + g
            means[s] = mean_of(row_of(pri_recv, table[0, s]), g)[0]

    parcels[segs] = jnp.zeros(parcels.shape[1:], F32)
    iota = lax.broadcasted_iota(jnp.int32, (8, points), 0)
    lanes = lax.broadcasted_iota(jnp.int32, (1, points), 1)
    steps = segs // total // GROUP
    for c in range(chunks):
        nodes = sec_recv[c]
        if c == 0:
            wait_send(req_send, req_recv, 0)
            wait_send(pri_send, pri_recv, 1)
        wait_recv(sec_send[c], nodes, 2 + c)
        if c == 0:
            for later in range(1, chunks):
                start_all(sec_send[later], sec_recv[later], 2 + later)

        @pl.loop(firsts[c] * steps, (firsts[c] + PHASES[c]) * steps)
        def _(i):
            group_values(nodes, lambda g: table[2, i * GROUP + g], lambda g: feats[table[1, i * GROUP + g]])
            for g in range(GROUP):
                s = table[1, i * GROUP + g]
                mean, inv = mean_of(row_of(nodes, table[2, i * GROUP + g]), g)
                w = jnp.where(lanes < counts[s], weights[pl.ds(s, 1), :], 0.0)
                diff = (mean - means[s]) * (w * inv)
                top = rounded(diff)
                gap_s[g] = jnp.where(iota < 4, top, diff - top)
            for g in range(GROUP):
                y = lax.dot_general(
                    gap_s[g].astype(BF16), both_s[g], (((1,), (1,)), ((), ())),
                    preferred_element_type=F32,
                )
                y = y[:, :n] + y[:, n:]
                parcels[i * GROUP + g] = y + pltpu.roll(y, 4, 0)

        def lift(p, dst):
            base = firsts[c] * quarter * devices + p * caps[c]
            for j in range(caps[c]):
                k = table[3, base + j]
                for d in range(3):
                    dst[p, d, j : j + 1, :] = parcels[k, d : d + 1, :]

        fill_and_start(lift, par_send[c], par_recv[c], 2 + chunks + c)

    for c in range(chunks):
        if c == chunks - 1:
            for k in range(chunks):
                wait_send(sec_send[k], sec_recv[k], 2 + k)
            for k in range(chunks - 1):
                wait_send(par_send[k], par_recv[k], 2 + chunks + k)
        wait_recv(par_send[c], par_recv[c], 2 + chunks + c)
        size = devices * caps[c]
        row = lax.broadcasted_iota(jnp.int32, (blocks, size), 0).astype(F32)
        select = jnp.where(row == hot[c : c + 1, :size], 1.0, 0.0).astype(BF16)
        for d in range(3):
            x = par_recv[c][:, d].reshape(size, n)
            top, mid, low = split_three(x)
            parts = jnp.concatenate([top, mid, low], axis=1).astype(BF16)
            y = jnp.dot(select, parts, preferred_element_type=F32)
            y = y[:, :n] + (y[:, n : 2 * n] + y[:, 2 * n :])
            gap[d] = y if c == 0 else gap[d] + y
    wait_send(par_send[-1], par_recv[-1], 1 + 2 * chunks)


def body(node_coords, node_disp, qpoints, qweights, qcount, sec_block, pri_block):
    devices = lax.axis_size("gx") * lax.axis_size("gy")
    blocks, comps, n = node_coords.shape
    segs, _, points = qpoints.shape
    cap = 2 * segs // devices
    width = 2 * comps * n
    caps = [m * cap // sum(PHASES) for m in PHASES]
    kinds = 2 + 2 * len(caps)
    vmem, smem = pl.BlockSpec(memory_space=pltpu.VMEM), pl.BlockSpec(memory_space=pltpu.SMEM)
    gap = pl.pallas_call(
        fused_kernel,
        out_shape=pltpu.VMEM((comps, blocks, n), F32),
        in_specs=[vmem, vmem, smem] + [pl.BlockSpec(memory_space=pltpu.HBM)] * 4,
        out_specs=vmem,
        scratch_shapes=[
            pltpu.VMEM((comps, blocks, n), F32),
            pltpu.VMEM((comps, blocks, n), F32),
            pltpu.VMEM((comps, segs, points), F32),
            pltpu.VMEM((segs, points), F32),
            pltpu.VMEM((segs, 48, points), BF16),
            pltpu.VMEM((devices, 1, 128), jnp.int32),
            pltpu.VMEM((devices, 1, 128), jnp.int32),
            pltpu.VMEM((devices, 128), F32),
            pltpu.SMEM((devices, 1, 128), jnp.int32),
            pltpu.VMEM((4, devices * cap), jnp.int32),
            pltpu.SMEM((4, devices * cap), jnp.int32),
            pltpu.VMEM((len(caps), devices * max(caps)), F32),
            pltpu.VMEM((devices, cap, width), F32),
            pltpu.VMEM((devices, cap, width), F32),
            pltpu.VMEM((segs, 8, points), F32),
            pltpu.VMEM((segs + 1, 8, n), F32),
            pltpu.VMEM((GROUP, 2 * n, points), BF16),
            pltpu.VMEM((GROUP, 8, points), F32),
            *[pltpu.VMEM((devices, m, width), F32) for m in caps + caps],
            *[pltpu.VMEM((devices, comps, m, n), F32) for m in caps + caps],
            pltpu.SemaphoreType.DMA((kinds,)),
            pltpu.SemaphoreType.DMA((kinds,)),
            pltpu.SemaphoreType.DMA((6,)),
        ],
        compiler_params=pltpu.CompilerParams(collective_id=0, has_side_effects=True),
        name="fused",
    )(
        pri_block, sec_block, qcount,
        node_coords.transpose(1, 0, 2), node_disp.transpose(1, 0, 2),
        qpoints.transpose(1, 0, 2), qweights,
    )
    return gap.transpose(1, 0, 2)


def solution(mesh):
    placed = (
        P(("gx", "gy"), None, None),
        P(("gx", "gy"), None, None),
        P(("gx", "gy"), None, None),
        P(("gx", "gy"), None),
        P(("gx", "gy")),
        P(("gx", "gy")),
        P(("gx", "gy")),
    )
    return jax.shard_map(
        body, mesh=mesh, in_specs=placed, out_specs=P(("gx", "gy"), None, None), check_vma=False
    )
```
